32 devices in a mesh: seqa: 8 (over z, x), seqb: 4 (over y, core).
Axes of the slice: x: 2, y: 2, z: 4, core: 2. Of those that a mesh axis runs over, the one named last changes fastest.
Arguments:
- queries: bfloat16 [16384, 4096], P(('seqa', 'seqb')), may hold values from -60 to 60
- keys: bfloat16 [16384, 1024], P(('seqa', 'seqb')), may hold values from -8 to 8
- values: bfloat16 [16384, 1024], P(('seqa', 'seqb')), may hold values from -6 to 6
- doc_start: int32 [16384], P(('seqa', 'seqb')), may hold values from 0 to 16383, as said below
Outputs:
- attended: bfloat16 [16384, 4096], P(('seqa', 'seqb'))
The draws below stay inside these ranges and needn't reach their ends.
Inputs may be any that keep to these rules, and one draw needn't show every extreme that they name: Never falling along the sequence, doc_start[i] <= i, the same value for all tokens of one document, and doc_start[0] = 0.
All inputs are finite; a program needn't handle non-finite values.
Results may differ from the reference program's by a relative error of at most 0.0038.
Values may be sent and summed in bfloat16 or wider, within the bound.
No kernel may reach another device: no remote copies, remote signals or barrier semaphores. Data moves between devices by JAX's collectives and lax.ppermute only.
A program may use at most 64 MiB of HBM per device.

```python
import math
import jax
import jax.numpy as jnp
from jax import lax

QUERY_HEADS = 32
KEY_VALUE_HEADS = 8
HEAD_SIZE = 128
TOK_DEV = 512
SEQUENCE_TOKENS = 16384


def query_key_pair(key):
    base = jax.random.fold_in(key, 11)
    query_key, key_random_seed = jax.random.split(base, 2)
    sampled_keys = jax.random.truncated_normal(key_random_seed, -6.0, 6.0, (SEQUENCE_TOKENS, KEY_VALUE_HEADS * HEAD_SIZE), jnp.float32)
    queries_drawn = jax.random.truncated_normal(query_key, -6.0, 6.0, (SEQUENCE_TOKENS, QUERY_HEADS * HEAD_SIZE), jnp.float32)
    return (queries_drawn, sampled_keys)


def draw_queries(key, part):
    return query_key_pair(key)[0].astype(jnp.bfloat16)


def draw_keys(key, part):
    return query_key_pair(key)[1].astype(jnp.bfloat16)


def draw_doc_start(key, part):
    marks = jax.random.randint(jax.random.fold_in(key, 3), (SEQUENCE_TOKENS,), 0, 2 * TOK_DEV)
    places = jnp.arange(SEQUENCE_TOKENS, dtype=jnp.int32)
    opening = (marks == 0) & (places >= 3 * TOK_DEV) | (places == 0)
    begins = jnp.where(opening, places, 0).astype(jnp.int32)
    return lax.cummax(begins, axis=0)


def shard_levels(own_key, shape, cuts, smallest, largest):
    def one(axis_at, parts):
        heights = jax.random.uniform(jax.random.fold_in(jax.random.fold_in(own_key, 6), axis_at), (parts,), jnp.float32, smallest / len(cuts), largest / len(cuts))
        return jnp.repeat(jnp.exp(heights), shape[axis_at] // parts).reshape((-1,) + (1,) * (len(shape) - axis_at - 1))

    gain = one(*cuts[0])
    for cut in cuts[1:]:
        gain = gain * one(*cut)
    return gain


def scatter_about(rng, shape, width, limit, shards=(), kind=jnp.bfloat16):
    loudness = shard_levels(rng, shape, shards, -0.22, 0.18) if shards else 1.0
    values = jax.random.normal(rng, shape, jnp.float32) * width * loudness
    return jnp.minimum(jnp.maximum(values, -limit), limit).astype(kind)


def setup_inputs(seed: int = 0) -> dict:
    arg_keys = jax.random.split(jax.random.key(seed), 5)
    queries = draw_queries(jax.random.fold_in(arg_keys[4], 71), 0)
    keys = draw_keys(jax.random.fold_in(arg_keys[4], 71), 0)
    values = scatter_about(arg_keys[2], (SEQUENCE_TOKENS, KEY_VALUE_HEADS * HEAD_SIZE), 1.0, 6.0, ((0, 32),))
    doc_start = draw_doc_start(jax.random.fold_in(arg_keys[4], 71), 0)
    return {"queries": queries, "keys": keys, "values": values, "doc_start": doc_start}


def reference(queries, keys, values, doc_start):
    rows_per_block = min(512, TOK_DEV)
    window_length = 2 * TOK_DEV
    group_width = QUERY_HEADS // KEY_VALUE_HEADS
    score_scale = 1.0 / math.sqrt(HEAD_SIZE)
    padded_keys = jnp.concatenate([jnp.zeros((window_length, KEY_VALUE_HEADS * HEAD_SIZE), jnp.bfloat16), keys], axis=0)
    padded_values = jnp.concatenate([jnp.zeros((window_length, KEY_VALUE_HEADS * HEAD_SIZE), jnp.bfloat16), values], axis=0)

    def one_block(block_index):
        offset = (block_index * rows_per_block).astype(jnp.int32)
        block_of_queries = lax.dynamic_slice_in_dim(queries, offset, rows_per_block, 0).astype(jnp.float32)
        block_of_queries = block_of_queries.reshape(rows_per_block, KEY_VALUE_HEADS, group_width, HEAD_SIZE)
        block_of_keys = lax.dynamic_slice_in_dim(padded_keys, offset, window_length + rows_per_block, 0).astype(jnp.float32)
        block_of_keys = block_of_keys.reshape(window_length + rows_per_block, KEY_VALUE_HEADS, HEAD_SIZE)
        block_of_values = lax.dynamic_slice_in_dim(padded_values, offset, window_length + rows_per_block, 0).astype(jnp.float32)
        block_of_values = block_of_values.reshape(window_length + rows_per_block, KEY_VALUE_HEADS, HEAD_SIZE)
        scores = jnp.einsum('thgd,khd->hgtk', block_of_queries, block_of_keys) * score_scale
        query_place = offset + jnp.arange(rows_per_block, dtype=jnp.int32)
        key_place = offset - window_length + jnp.arange(window_length + rows_per_block, dtype=jnp.int32)
        starts = lax.dynamic_slice_in_dim(doc_start, offset, rows_per_block, 0)
        visible = (key_place[None, :] <= query_place[:, None]) & (key_place[None, :] > query_place[:, None] - window_length) & (key_place[None, :] >= starts[:, None])
        scores = jnp.where(visible[None, None], scores, jnp.float32(-1e+30))
        row_top = lax.optimization_barrier(jnp.max(scores, axis=-1, keepdims=True))
        exponent = jnp.where(visible[None, None], jnp.exp(scores - row_top), jnp.float32(0.0))
        row_sum = lax.optimization_barrier(jnp.sum(exponent, axis=-1, keepdims=True))
        weights = exponent.astype(jnp.bfloat16).astype(jnp.float32)
        summed = jnp.einsum('hgtk,khd->thgd', weights, block_of_values)
        result = summed / jnp.transpose(row_sum, (2, 0, 1, 3))
        return result.reshape(rows_per_block, QUERY_HEADS * HEAD_SIZE).astype(jnp.bfloat16)
    blocks = lax.map(one_block, jnp.arange(SEQUENCE_TOKENS // rows_per_block, dtype=jnp.int32))
    return blocks.reshape(SEQUENCE_TOKENS, QUERY_HEADS * HEAD_SIZE)
```

```python
import functools
import math

import jax
import jax.numpy as jnp
from jax import lax
from jax.experimental import pallas as pl
from jax.experimental.pallas import tpu as pltpu
from jax.sharding import PartitionSpec as P

HEAD_SIZE = 128
ROWS = 128
AXES = ("seqa", "seqb")
HIDDEN = -1e30


def attend_kernel(place, starts, q, k2, v2, k1, v1, k0, v0, *rest):
    out, bias = rest[-2], rest[-1]
    shard = q.shape[0]
    head = k0.shape[1]
    group = q.shape[1] // head
    window = 2 * shard
    width = window + ROWS
    blocks = shard // ROWS
    factor = math.log2(math.e) / math.sqrt(head)

    @pl.when(pl.program_id(0) == 0)
    def _():
        for b in range(blocks):
            row = lax.broadcasted_iota(jnp.int32, (ROWS, width), 0) + b * ROWS
            col = lax.broadcasted_iota(jnp.int32, (ROWS, width), 1) + (b * ROWS - window)
            start = starts[b * ROWS : (b + 1) * ROWS, :] - place[0]
            visible = (col <= row) & (col > row - window) & (col >= start)
            bias[b] = jnp.where(visible, jnp.float32(0.0), jnp.float32(HIDDEN))

    ones = jnp.ones((width, head), jnp.bfloat16)
    for b in range(blocks):
        lo, hi = b * ROWS, (b + 1) * ROWS
        keys = jnp.concatenate([k2[lo:, :], k1[...], k0[:hi, :]], axis=0)
        vals = jnp.concatenate([v2[lo:, :], v1[...], v0[:hi, :]], axis=0)
        vals = jnp.concatenate([vals, ones], axis=1)
        for g in range(group):
            qg = q[lo:hi, g * head : (g + 1) * head]
            s = lax.dot_general(qg, keys, (((1,), (1,)), ((), ())), preferred_element_type=jnp.float32)
            s = s + bias[b]
            top = jnp.max(s, axis=-1, keepdims=True)
            w = jnp.exp2((s - top) * factor).astype(jnp.bfloat16)
            o = lax.dot_general(w, vals, (((1,), (0,)), ((), ())), preferred_element_type=jnp.float32)
            out[lo:hi, g * head : (g + 1) * head] = (o[:, :head] / o[:, head:]).astype(jnp.bfloat16)


def attend(place, starts, queries, second, first, keys, values, partial, h0, n):
    shard = queries.shape[0]
    group = queries.shape[1] // keys.shape[1]
    head = HEAD_SIZE
    kv = lambda f: pl.BlockSpec((shard, head), f)
    wide = pl.BlockSpec((shard, group * head), lambda j: (0, h0 + j))
    in_specs = [
        pl.BlockSpec(memory_space=pltpu.SMEM),
        pl.BlockSpec((shard, 1), lambda j: (0, 0)),
        wide,
        kv(lambda j: (0, j)),
        kv(lambda j: (0, n + j)),
        kv(lambda j: (0, j)),
        kv(lambda j: (0, n + j)),
        kv(lambda j: (0, h0 + j)),
        kv(lambda j: (0, h0 + j)),
    ]
    args = [place, starts, queries, second, second, first, first, keys, values]
    aliases = {}
    if partial is not None:
        in_specs.append(pl.BlockSpec(memory_space=pl.ANY))
        aliases = {len(args): 0}
        args.append(partial)
    width = 2 * shard + ROWS
    return pl.pallas_call(
        attend_kernel,
        grid=(n,),
        in_specs=in_specs,
        out_specs=wide,
        out_shape=jax.ShapeDtypeStruct(queries.shape, queries.dtype),
        scratch_shapes=[pltpu.VMEM((shard // ROWS, ROWS, width), jnp.float32)],
        input_output_aliases=aliases,
        compiler_params=pltpu.CompilerParams(dimension_semantics=("arbitrary",)),
        cost_estimate=pl.CostEstimate(
            flops=n * group * shard * width * head * 6,
            transcendentals=n * group * shard * width,
            bytes_accessed=n * head * shard * 2 * (2 * group + 6),
        ),
        name="attend",
    )(*args)


def chunk_sizes(heads):
    sizes = []
    left = heads
    while left:
        n = min(left, 2 if left > 2 else 1)
        sizes.append(n)
        left -= n
    return sizes


def local(queries, keys, values, doc_start):
    shard = queries.shape[0]
    head = HEAD_SIZE
    heads = keys.shape[1] // head
    count = lax.axis_size(AXES)
    me = lax.axis_index(AXES)
    ahead = [(i, i + 2) for i in range(count - 2)]
    swap = [(i, i ^ 1) for i in range(count)]
    place = (me * shard).astype(jnp.int32).reshape(1)
    starts = doc_start.reshape(shard, 1)
    even = me % 2 == 0

    sent, spans, h0 = [], [], 0
    for n in chunk_sizes(heads):
        cols = slice(h0 * head, (h0 + n) * head)
        sent.append(jnp.concatenate([keys[:, cols], values[:, cols]], axis=1))
        spans.append((h0, n))
        h0 += n
    out = None
    for chunk, (h0, n) in zip(sent, spans):
        second = lax.ppermute(chunk, AXES, ahead)
        if out is not None:
            second, out = lax.optimization_barrier((second, out))
        first = lax.ppermute(jnp.where(even, chunk, second), AXES, swap)
        out = attend(place, starts, queries, second, first, keys, values, out, h0, n)
    return out


def solution(mesh):
    return jax.shard_map(
        local,
        mesh=mesh,
        in_specs=(P(AXES, None), P(AXES, None), P(AXES, None), P(AXES)),
        out_specs=P(AXES, None),
        check_vma=False,
    )
```

```python
import math

import jax
import jax.numpy as jnp
from jax import lax
from jax.experimental import pallas as pl
from jax.experimental.pallas import tpu as pltpu
from jax.sharding import PartitionSpec as P


HEAD_SIZE = 128
ROWS = 128
AXES = ("seqa", "seqb")
HIDDEN = -1e30


def attend_kernel(place, starts, q, k2, v2, k1, v1, k0, v0, *rest):
    out, bias = rest[-2], rest[-1]
    shard = q.shape[0]
    head = k0.shape[1]
    group = q.shape[1] // head
    window = 2 * shard
    width = window + ROWS
    blocks = shard // ROWS
    factor = math.log2(math.e) / math.sqrt(head)

    @pl.when(pl.program_id(0) == 0)
    def _():
        for b in range(blocks):
            row = lax.broadcasted_iota(jnp.int32, (ROWS, width), 0) + b * ROWS
            col = lax.broadcasted_iota(jnp.int32, (ROWS, width), 1) + (b * ROWS - window)
            start = starts[b * ROWS : (b + 1) * ROWS, :] - place[0]
            visible = (col <= row) & (col > row - window) & (col >= start)
            bias[b] = jnp.where(visible, jnp.float32(0.0), jnp.float32(HIDDEN))

    ones = jnp.ones((width, head), jnp.bfloat16)
    for b in range(blocks):
        lo, hi = b * ROWS, (b + 1) * ROWS
        keys = jnp.concatenate([k2[lo:, :], k1[...], k0[:hi, :]], axis=0)
        vals = jnp.concatenate([v2[lo:, :], v1[...], v0[:hi, :]], axis=0)
        vals = jnp.concatenate([vals, ones], axis=1)
        qs = jnp.concatenate([q[lo:hi, g * head : (g + 1) * head] for g in range(group)], axis=0)
        s = lax.dot_general(qs, keys, (((1,), (1,)), ((), ())), preferred_element_type=jnp.float32)
        ws = []
        for g in range(group):
            sg = s[g * ROWS : (g + 1) * ROWS, :] + bias[b]
            top = jnp.max(sg, axis=-1, keepdims=True)
            ws.append(jnp.exp2((sg - top) * factor).astype(jnp.bfloat16))
        w = jnp.concatenate(ws, axis=0)
        o = lax.dot_general(w, vals, (((1,), (0,)), ((), ())), preferred_element_type=jnp.float32)
        o = (o[:, :head] / o[:, head:]).astype(jnp.bfloat16)
        for g in range(group):
            out[lo:hi, g * head : (g + 1) * head] = o[g * ROWS : (g + 1) * ROWS, :]


def attend(place, starts, queries, second, first, keys, values, partial, h0, n):
    shard = queries.shape[0]
    group = queries.shape[1] // keys.shape[1]
    head = HEAD_SIZE
    kv = lambda f: pl.BlockSpec((shard, head), f)
    wide = pl.BlockSpec((shard, group * head), lambda j: (0, h0 + j))
    in_specs = [
        pl.BlockSpec(memory_space=pltpu.SMEM),
        pl.BlockSpec((shard, 1), lambda j: (0, 0)),
        wide,
        kv(lambda j: (0, j)),
        kv(lambda j: (0, n + j)),
        kv(lambda j: (0, j)),
        kv(lambda j: (0, n + j)),
        kv(lambda j: (0, h0 + j)),
        kv(lambda j: (0, h0 + j)),
    ]
    args = [place, starts, queries, second, second, first, first, keys, values]
    aliases = {}
    if partial is not None:
        in_specs.append(pl.BlockSpec(memory_space=pl.ANY))
        aliases = {len(args): 0}
        args.append(partial)
    width = 2 * shard + ROWS
    return pl.pallas_call(
        attend_kernel,
        grid=(n,),
        in_specs=in_specs,
        out_specs=wide,
        out_shape=jax.ShapeDtypeStruct(queries.shape, queries.dtype),
        scratch_shapes=[pltpu.VMEM((shard // ROWS, ROWS, width), jnp.float32)],
        input_output_aliases=aliases,
        compiler_params=pltpu.CompilerParams(dimension_semantics=("arbitrary",)),
        cost_estimate=pl.CostEstimate(
            flops=n * group * shard * width * head * 6,
            transcendentals=n * group * shard * width,
            bytes_accessed=n * head * shard * 2 * (2 * group + 6),
        ),
        name="attend",
    )(*args)


def chunk_sizes(heads):
    sizes, left = [], heads
    while left:
        n = max(1, -(-left * 3 // 8))
        sizes.append(n)
        left -= n
    return sizes


def layer(queries, keys, values, doc_start):
    shard = queries.shape[0]
    head = HEAD_SIZE
    heads = keys.shape[1] // head
    count = lax.axis_size(AXES)
    me = lax.axis_index(AXES)
    ahead = [(i, i + 2) for i in range(count - 2)]
    swap = [(i, i ^ 1) for i in range(count)]
    place = (me * shard).astype(jnp.int32).reshape(1)
    starts = doc_start.reshape(shard, 1)
    even = me % 2 == 0

    sent, spans, h0 = [], [], 0
    for n in chunk_sizes(heads):
        cols = slice(h0 * head, (h0 + n) * head)
        sent.append(jnp.concatenate([keys[:, cols], values[:, cols]], axis=1))
        spans.append((h0, n))
        h0 += n
    out = None
    for chunk, (h0, n) in zip(sent, spans):
        second = lax.ppermute(chunk, AXES, ahead)
        if out is not None:
            second, out = lax.optimization_barrier((second, out))
        first = lax.ppermute(jnp.where(even, chunk, second), AXES, swap)
        out = attend(place, starts, queries, second, first, keys, values, out, h0, n)
    return out


def solution(mesh):
    return jax.shard_map(
        layer,
        mesh=mesh,
        in_specs=(P(AXES, None), P(AXES, None), P(AXES, None), P(AXES)),
        out_specs=P(AXES, None),
        check_vma=False,
    )
```

```python
import math

import jax
import jax.numpy as jnp
from jax import lax
from jax.experimental import pallas as pl
from jax.experimental.pallas import tpu as pltpu
from jax.sharding import PartitionSpec as P


HEAD_SIZE = 128
ROWS = 128
AXES = ("seqa", "seqb")
HIDDEN = -1e30


def attend_kernel(place, starts, q, k2, v2, k1, v1, k0, v0, *rest):
    out, bias = rest[-2], rest[-1]
    shard = q.shape[0]
    head = k0.shape[1]
    group = q.shape[1] // head
    window = 2 * shard
    width = window + ROWS
    blocks = shard // ROWS
    factor = math.log2(math.e) / math.sqrt(head)

    @pl.when(pl.program_id(0) == 0)
    def _():
        for b in range(blocks):
            row = lax.broadcasted_iota(jnp.int32, (ROWS, width), 0) + b * ROWS
            col = lax.broadcasted_iota(jnp.int32, (ROWS, width), 1) + (b * ROWS - window)
            start = starts[b * ROWS : (b + 1) * ROWS, :] - place[0]
            visible = (col <= row) & (col > row - window) & (col >= start)
            bias[b] = jnp.where(visible, jnp.float32(0.0), jnp.float32(HIDDEN))

    ones = jnp.ones((width, head), jnp.bfloat16)
    for b in range(blocks):
        lo, hi = b * ROWS, (b + 1) * ROWS
        keys = jnp.concatenate([k2[lo:, :], k1[...], k0[:hi, :]], axis=0)
        vals = jnp.concatenate([v2[lo:, :], v1[...], v0[:hi, :]], axis=0)
        vals = jnp.concatenate([vals, ones], axis=1)
        qs = jnp.concatenate([q[lo:hi, g * head : (g + 1) * head] for g in range(group)], axis=0)
        s = lax.dot_general(qs, keys, (((1,), (1,)), ((), ())), preferred_element_type=jnp.float32)
        ws = []
        for g in range(group):
            sg = s[g * ROWS : (g + 1) * ROWS, :] + bias[b]
            top = jnp.max(sg, axis=-1, keepdims=True)
            ws.append(jnp.exp2((sg - top) * factor).astype(jnp.bfloat16))
        w = jnp.concatenate(ws, axis=0)
        o = lax.dot_general(w, vals, (((1,), (0,)), ((), ())), preferred_element_type=jnp.float32)
        o = (o[:, :head] / o[:, head:]).astype(jnp.bfloat16)
        for g in range(group):
            out[lo:hi, g * head : (g + 1) * head] = o[g * ROWS : (g + 1) * ROWS, :]


def attend(place, starts, queries, second, first, keys, values, partial, h0, n):
    shard = queries.shape[0]
    group = queries.shape[1] // keys.shape[1]
    head = HEAD_SIZE
    kv = lambda f: pl.BlockSpec((shard, head), f)
    wide = pl.BlockSpec((shard, group * head), lambda j: (0, h0 + j))
    in_specs = [
        pl.BlockSpec(memory_space=pltpu.SMEM),
        pl.BlockSpec((shard, 1), lambda j: (0, 0)),
        wide,
        kv(lambda j: (0, j)),
        kv(lambda j: (0, n + j)),
        kv(lambda j: (0, j)),
        kv(lambda j: (0, n + j)),
        kv(lambda j: (0, h0 + j)),
        kv(lambda j: (0, h0 + j)),
    ]
    args = [place, starts, queries, second, second, first, first, keys, values]
    aliases = {}
    if partial is not None:
        in_specs.append(pl.BlockSpec(memory_space=pl.ANY))
        aliases = {len(args): 0}
        args.append(partial)
    width = 2 * shard + ROWS
    return pl.pallas_call(
        attend_kernel,
        grid=(n,),
        in_specs=in_specs,
        out_specs=wide,
        out_shape=jax.ShapeDtypeStruct(queries.shape, queries.dtype),
        scratch_shapes=[pltpu.VMEM((shard // ROWS, ROWS, width), jnp.float32)],
        input_output_aliases=aliases,
        compiler_params=pltpu.CompilerParams(dimension_semantics=("arbitrary",)),
        cost_estimate=pl.CostEstimate(
            flops=n * group * shard * width * head * 6,
            transcendentals=n * group * shard * width,
            bytes_accessed=n * head * shard * 2 * (2 * group + 6),
        ),
        name="attend",
    )(*args)


def chunk_sizes(heads):
    lead = heads // 4
    half = (heads - lead) // 2
    return [lead, half, heads - lead - half]


def layer(queries, keys, values, doc_start):
    shard = queries.shape[0]
    head = HEAD_SIZE
    heads = keys.shape[1] // head
    count = lax.axis_size(AXES)
    me = lax.axis_index(AXES)
    ahead = [(i, i + 2) for i in range(count - 2)]
    swap = [(i, i ^ 1) for i in range(count)]
    place = (me * shard).astype(jnp.int32).reshape(1)
    starts = doc_start.reshape(shard, 1)
    even = me % 2 == 0

    sent, spans, h0 = [], [], 0
    for n in chunk_sizes(heads):
        cols = slice(h0 * head, (h0 + n) * head)
        sent.append(jnp.concatenate([keys[:, cols], values[:, cols]], axis=1))
        spans.append((h0, n))
        h0 += n
    out = None
    for chunk, (h0, n) in zip(sent, spans):
        second = lax.ppermute(chunk, AXES, ahead)
        if out is not None:
            second, out = lax.optimization_barrier((second, out))
        first = lax.ppermute(jnp.where(even, chunk, second), AXES, swap)
        out = attend(place, starts, queries, second, first, keys, values, out, h0, n)
    return out


def solution(mesh):
    return jax.shard_map(
        layer,
        mesh=mesh,
        in_specs=(P(AXES, None), P(AXES, None), P(AXES, None), P(AXES)),
        out_specs=P(AXES, None),
        check_vma=False,
    )
```
